32 devices in a mesh: facet: 4 (over z), sub: 2 (over y), wa: 4 (over x, core).
Axes of the slice: x: 2, y: 2, z: 4, core: 2. Of those that a mesh axis runs over, the one named last changes fastest.
Arguments:
- facet_data: bfloat16 [4, 128, 2, 8192], P('facet', ('sub', 'wa')), may hold values from -6 to 6
- window: float32 [8192], replicated, may hold values from 0.1 to 1
- screen_phase: float32 [1024, 1024], P('facet'), may hold values from -0.5 to 0.5
- facet_shift: int32 [4], replicated, may hold values from 0 to 1023
- sub_offset: int32 [8], replicated, may hold values from 0 to 8191
- win_start: int32 [4, 8], replicated, may hold values from 0 to 512
- win_extent: int32 [4, 8], replicated, may hold values from 256 to 512, as said below
- owner_slot: int32 [8], replicated, may hold values from 0 to 7, each once
- layer_w: int32 [8], replicated, may hold values from -12 to 12
Outputs:
- layers: bfloat16 [8, 8, 1024, 2, 1024], P('sub', 'wa', 'facet')
The draws below stay inside these ranges and needn't reach their ends.
Inputs may be any that keep to these rules, and one draw needn't show every extreme that they name: win_start[f, j] + win_extent[f, j] <= 1024 for every facet f and subgrid j. A permutation of the subgrids; the subgrid with owner_slot = p belongs to sub index p // 4.
All inputs are finite; a program needn't handle non-finite values.
Results may differ from the reference program's by a relative error of at most 0.008.
Values may be sent and summed in bfloat16 or wider, within the bound.
A program may use at most 128 MiB of HBM per device.

```python
import math
import jax
import jax.numpy as jnp
from jax import lax

FN = 8192
SG = 1024
NFAC = 4
SUBS = 8
LAYERS = 8
STRIP = 128
EMAX = 512
EMIN = 256


def draw_win_extent(key, part):
    base_key = jax.random.fold_in(key, 11)
    first_key, second_key, third_key = jax.random.split(base_key, 3)
    values = jax.random.randint(first_key, (NFAC, SUBS), EMIN, EMAX + 1)
    chosen = jax.random.randint(second_key, (NFAC,), 0, SUBS)
    column = jax.random.randint(third_key, (), 0, SUBS)
    indices = jnp.arange(SUBS)
    widest = (indices[None, :] == chosen[:, None]) | (indices[None, :] == column)
    return jnp.where(widest, EMAX, values).astype(jnp.int32)


def place_ends(result, key, smallest, largest):
    dims = result.shape
    place = [jax.random.randint(jax.random.fold_in(key, axis), (), 0, dims[axis]) for axis in range(len(dims))]
    result = result.at[tuple(place)].set(smallest)
    longest = dims.index(max(dims))
    place[longest] = (place[longest] + 1) % dims[longest]
    return result.at[tuple(place)].set(largest)


def levels(rng, extent, cuts, low, high):
    def one(dim, parts):
        steps = jax.random.uniform(jax.random.fold_in(jax.random.fold_in(rng, 6), dim), (parts,), jnp.float32, low / len(cuts), high / len(cuts))
        return jnp.repeat(jnp.exp(steps), extent[dim] // parts).reshape((-1,) + (1,) * (len(extent) - dim - 1))

    gain = one(*cuts[0])
    for cut in cuts[1:]:
        gain = gain * one(*cut)
    return gain


def noise(stream_key, extent, scale, most, shards=(), kind=jnp.bfloat16):
    values = scale * jax.random.normal(stream_key, extent, jnp.float32)
    if shards:
        values = values * levels(stream_key, extent, shards, -0.22, 0.18)
    return jnp.clip(values, -most, most).astype(kind)


def setup_inputs(seed: int = 0) -> dict:
    key_list = jax.random.split(jax.random.key(seed), 10)
    return {
        "facet_data": noise(key_list[0], (NFAC, STRIP, 2, FN), 1.0, 6.0, ((0, 4), (1, 8))),
        "window": jnp.clip(jnp.exp(jax.random.uniform(key_list[1], (FN,), jnp.float32, math.log(0.1), math.log(1.0))), 0.1, 1.0),
        "screen_phase": jnp.clip(jax.random.uniform(key_list[2], (SG, SG), jnp.float32, -0.5, 0.5) * levels(key_list[2], (SG, SG), ((0, 4),), -0.4, 0.0), -0.5, 0.5),
        "facet_shift": place_ends(jax.random.randint(key_list[3], (NFAC,), 0, SG), jax.random.fold_in(key_list[3], 1), 0, SG - 1).astype(jnp.int32),
        "sub_offset": place_ends(jax.random.randint(key_list[4], (SUBS,), 0, FN), jax.random.fold_in(key_list[4], 1), 0, FN - 1).astype(jnp.int32),
        "win_start": place_ends(jax.random.randint(key_list[5], (NFAC, SUBS), 0, SG - EMAX + 1), jax.random.fold_in(key_list[5], 1), 0, SG - EMAX).astype(jnp.int32),
        "win_extent": draw_win_extent(jax.random.fold_in(key_list[9], 71), 0),
        "owner_slot": jax.random.permutation(key_list[7], SUBS).astype(jnp.int32),
        "layer_w": place_ends(jax.random.randint(key_list[8], (LAYERS,), -12, 13), jax.random.fold_in(key_list[8], 1), -12, 12).astype(jnp.int32),
    }


def phase_of(products, modulus, sign_value):
    angles = sign_value * 2.0 * math.pi / modulus * (products % modulus).astype(jnp.float32)
    return (jnp.cos(angles), jnp.sin(angles))

def phase_pair(row_ids, col_ids, modulus, sign_value):
    return phase_of(row_ids[:, None] * col_ids[None, :], modulus, sign_value)

def held_bf16(values):
    return lax.optimization_barrier(values.astype(jnp.bfloat16)).astype(jnp.float32)

def precise_dot(left, right):
    return jnp.dot(left, right, precision=lax.Precision.HIGHEST)

def reference(facet_data, window, screen_phase, facet_shift, sub_offset, win_start, win_extent, owner_slot, layer_w):
    signal = facet_data.astype(jnp.float32) * window
    spectrum = jnp.fft.fft(signal[:, :, 0] + 1j * signal[:, :, 1], axis=-1) / math.sqrt(FN)
    columns = jnp.arange(SG, dtype=jnp.int32)
    shift_cos, shift_sin = phase_pair(facet_shift, columns, SG, 1.0)
    strip_ids = jnp.arange(STRIP, dtype=jnp.int32)
    row_cos, row_sin = phase_pair(columns, strip_ids, SG, -1.0)
    row_cos = held_bf16(row_cos)
    row_sin = held_bf16(row_sin)
    fwd_cos, fwd_sin = phase_pair(columns, columns, SG, -1.0)
    fwd_cos = held_bf16(fwd_cos)
    fwd_sin = held_bf16(fwd_sin)

    def one_subgrid(sub_index):
        picked = jnp.take(spectrum, (sub_offset[sub_index] + columns) % FN, axis=2)
        begin_col = win_start[:, sub_index][:, None]
        end_col = begin_col + win_extent[:, sub_index][:, None]
        inside = (columns[None, :] >= begin_col) & (columns[None, :] < end_col)
        part_real = picked.real * shift_cos[:, None, :] - picked.imag * shift_sin[:, None, :]
        part_imag = picked.real * shift_sin[:, None, :] + picked.imag * shift_cos[:, None, :]
        part_real = held_bf16(jnp.where(inside[:, None, :], part_real, 0.0))
        part_imag = held_bf16(jnp.where(inside[:, None, :], part_imag, 0.0))
        summed = (lax.optimization_barrier(jnp.sum(part_real, 0)) + 1j * lax.optimization_barrier(jnp.sum(part_imag, 0))) / math.sqrt(NFAC)
        col_image = jnp.fft.ifft(summed, axis=-1) * math.sqrt(SG)
        q_real = held_bf16(col_image.real)
        q_imag = held_bf16(col_image.imag)
        p_real = (precise_dot(row_cos, q_real) - precise_dot(row_sin, q_imag)) / math.sqrt(STRIP)
        p_imag = (precise_dot(row_sin, q_real) + precise_dot(row_cos, q_imag)) / math.sqrt(STRIP)
        p_real = held_bf16(p_real)
        p_imag = held_bf16(p_imag)

        def one_layer(layer_value):
            turn_angles = layer_value.astype(jnp.float32) * screen_phase
            turn_cos = jnp.cos(turn_angles)
            turn_sin = jnp.sin(turn_angles)
            s_real = held_bf16(p_real * turn_cos - p_imag * turn_sin)
            s_imag = held_bf16(p_real * turn_sin + p_imag * turn_cos)
            o_real = precise_dot(s_real, fwd_cos) - precise_dot(s_imag, fwd_sin)
            o_imag = precise_dot(s_real, fwd_sin) + precise_dot(s_imag, fwd_cos)
            return (jnp.stack([o_real, o_imag], 1) / math.sqrt(SG)).astype(jnp.bfloat16)
        return lax.map(one_layer, layer_w)
    per_subgrid = lax.map(one_subgrid, jnp.arange(SUBS, dtype=jnp.int32))
    return jnp.zeros_like(per_subgrid).at[owner_slot].set(per_subgrid)
```

```python
import functools
import math

import jax
import jax.numpy as jnp
import numpy as np
from jax import lax
from jax.experimental import pallas as pl
from jax.experimental.pallas import tpu as pltpu
from jax.sharding import PartitionSpec as P

RADIX = 4


def table(products, modulus, sign_value):
    angles = (sign_value * 2.0 * math.pi / modulus) * (products % modulus).astype(np.float64)
    return np.cos(angles), np.sin(angles)


def wave(products, modulus):
    angles = (2.0 * math.pi / modulus) * (products % modulus).astype(jnp.float32)
    return jnp.cos(angles), jnp.sin(angles)


def high(form, left, right):
    return jnp.einsum(form, left, right, precision=lax.Precision.HIGH)


def facet_spectrum(signal):
    strip_rows = signal.shape[0]
    facet_len = signal.shape[2]
    inner_len = 128
    outer_len = facet_len // inner_len
    grid_in = signal.reshape(strip_rows, 2 * outer_len, inner_len)
    outer_ids = np.arange(outer_len)
    inner_ids = np.arange(inner_len)
    c1, s1 = table(outer_ids[:, None] * outer_ids[None, :], outer_len, -1.0)
    first = np.block([[c1, -s1], [s1, c1]]).astype(np.float32)
    mid = high("zy,ryq->rzq", jnp.asarray(first), grid_in)
    mid_real = mid[:, :outer_len]
    mid_imag = mid[:, outer_len:]
    ct, st = table(outer_ids[:, None] * inner_ids[None, :], facet_len, -1.0)
    ct = jnp.asarray(ct.astype(np.float32))
    st = jnp.asarray(st.astype(np.float32))
    turned_real = mid_real * ct - mid_imag * st
    turned_imag = mid_real * st + mid_imag * ct
    turned = jnp.concatenate([turned_real, turned_imag], 2)
    c2, s2 = table(inner_ids[:, None] * inner_ids[None, :], inner_len, -1.0)
    scale = 1.0 / math.sqrt(facet_len)
    second = (np.block([[c2, s2], [-s2, c2]]) * scale).astype(np.float32)
    out = high("rpn,nq->rqp", turned, jnp.asarray(second))
    return out.reshape(strip_rows, 2, facet_len)


def finish_kernel(band, count, scale_rows, left_ref, right_ref, cos_ref, sin_ref, fwd_ref, out_ref, held):
    layer = pl.program_id(1)
    grid_size = cos_ref.shape[2]
    part = grid_size // RADIX

    @pl.when(layer == 0)
    def _():
        rows = jnp.dot(left_ref[...], right_ref[...], preferred_element_type=jnp.float32)
        held[...] = (rows * scale_rows).astype(jnp.bfloat16)

    real = held[:band, :].astype(jnp.float32)
    imag = held[band:, :].astype(jnp.float32)
    cos = cos_ref[0]
    sin = sin_ref[0]
    s_real = (real * cos - imag * sin).astype(jnp.bfloat16)
    s_imag = (real * sin + imag * cos).astype(jnp.bfloat16)
    pieces = []
    for p in range(RADIX):
        lo, hi = p * part, (p + 1) * part
        pair = jnp.concatenate([s_real[:, lo:hi], s_imag[:, lo:hi]], 1)
        got = jnp.dot(pair, fwd_ref[p], preferred_element_type=jnp.float32)
        pieces.append((got[:, :part], got[:, part:]))
    (ar, ai), (br, bi), (cr, ci), (dr, di) = pieces
    er, ei, fr, fi = ar + cr, ai + ci, ar - cr, ai - ci
    gr, gi, hr, hi_ = br + dr, bi + di, br - dr, bi - di
    reals = jnp.concatenate([er + gr, fr + hi_, er - gr, fr - hi_], 1)
    imags = jnp.concatenate([ei + gi, fi - hr, ei - gi, fi + hr], 1)
    out_ref[0, 0, :, 0, :] = reals.astype(jnp.bfloat16)
    out_ref[0, 0, :, 1, :] = imags.astype(jnp.bfloat16)


def finish(left, right, cos, sin, forward, slots, scale_rows):
    layers, band, grid_size = cos.shape
    count = right.shape[0]
    return pl.pallas_call(
        functools.partial(finish_kernel, band, count, scale_rows),
        grid=(slots, layers),
        out_shape=jax.ShapeDtypeStruct((slots, layers, band, 2, grid_size), jnp.bfloat16),
        in_specs=[
            pl.BlockSpec((2 * band, count), lambda s, l: (0, 0)),
            pl.BlockSpec((count, grid_size), lambda s, l: (0, s)),
            pl.BlockSpec((1, band, grid_size), lambda s, l: (l, 0, 0)),
            pl.BlockSpec((1, band, grid_size), lambda s, l: (l, 0, 0)),
            pl.BlockSpec(forward.shape, lambda s, l: (0, 0, 0)),
        ],
        out_specs=pl.BlockSpec((1, 1, band, 2, grid_size), lambda s, l: (s, l, 0, 0, 0)),
        scratch_shapes=[pltpu.VMEM((2 * band, grid_size), jnp.bfloat16)],
        compiler_params=pltpu.CompilerParams(vmem_limit_bytes=48 * 1024 * 1024),
        cost_estimate=pl.CostEstimate(flops=10_000_000_000, bytes_accessed=20_000_000, transcendentals=0),
    )(left, right, cos, sin, forward)


def local(
    facet_data,
    window,
    screen_phase,
    facet_shift,
    sub_offset,
    win_start,
    win_extent,
    owner_slot,
    layer_w,
):
    facets = lax.axis_size("facet")
    owners = lax.axis_size("sub")
    teams = lax.axis_size("wa")
    facet_id = lax.axis_index("facet")
    team_id = lax.axis_index("wa")
    strip_rows = facet_data.shape[1]
    facet_len = facet_data.shape[3]
    band = screen_phase.shape[0]
    grid_size = screen_phase.shape[1]
    width = grid_size // 2
    part = grid_size // RADIX
    total_subs = owner_slot.shape[0]
    slots = total_subs // owners
    share = strip_rows // facets
    strip_total = strip_rows * owners * teams

    spectrum = facet_spectrum(facet_data[0].astype(jnp.float32) * window)
    slot_ids = jnp.arange(total_subs, dtype=jnp.int32)
    chooser = (owner_slot[None, :] == slot_ids[:, None]).astype(jnp.int32)
    offset_slot = jnp.sum(chooser * sub_offset[None, :], axis=1)
    start_all = jnp.sum(win_start[:, None, :] * chooser[None], axis=2)
    extent_all = jnp.sum(win_extent[:, None, :] * chooser[None], axis=2)
    start_mine = lax.dynamic_index_in_dim(start_all, facet_id, 0, keepdims=False)
    extent_mine = lax.dynamic_index_in_dim(extent_all, facet_id, 0, keepdims=False)
    shift_value = lax.dynamic_index_in_dim(facet_shift, facet_id, 0, keepdims=False)
    begin = (offset_slot + start_mine) % facet_len
    steps = jnp.arange(width, dtype=jnp.int32)
    turn_cos, turn_sin = wave(shift_value * (start_mine[:, None] + steps[None, :]), grid_size)
    inside = steps[None, :] < extent_mine[:, None]
    turn_cos = jnp.where(inside, turn_cos, 0.0)
    turn_sin = jnp.where(inside, turn_sin, 0.0)
    wrapped = jnp.concatenate([spectrum, spectrum[:, :, :width]], 2)
    cuts = []
    for j in range(total_subs):
        picked = lax.dynamic_slice_in_dim(wrapped, begin[j], width, 2)
        cos_j = turn_cos[j][None, :]
        sin_j = turn_sin[j][None, :]
        cuts.append(
            jnp.concatenate(
                [
                    picked[:, 0] * cos_j - picked[:, 1] * sin_j,
                    picked[:, 0] * sin_j + picked[:, 1] * cos_j,
                ],
                1,
            ).astype(jnp.bfloat16)
        )
    sendable = jnp.stack(cuts).reshape(owners, slots, facets, share, 2 * width)
    sendable = sendable.transpose(2, 0, 1, 3, 4).reshape(facets * owners, slots * share, 2 * width)
    received = lax.all_to_all(sendable, ("facet", "sub"), split_axis=0, concat_axis=0, tiled=True)

    v_ids = np.arange(part)[None, :] * RADIX + np.arange(RADIX)[:, None]
    back_cos, back_sin = table(np.arange(width)[:, None] * v_ids.reshape(1, -1), grid_size, 1.0)
    back = np.block([[back_cos, back_sin], [-back_sin, back_cos]])
    moved = jnp.dot(
        received.reshape(facets * owners * slots * share, 2 * width),
        jnp.asarray(back.astype(jnp.bfloat16)),
        preferred_element_type=jnp.float32,
    ).reshape(facets, owners, slots, share, 2, grid_size)
    my_slot = lax.axis_index("sub") * slots
    start_slot = lax.dynamic_slice_in_dim(start_all, my_slot, slots, 1)
    ramp_cos, ramp_sin = wave(
        start_slot[:, :, None] * jnp.asarray(v_ids.reshape(1, 1, -1).astype(np.int32)), grid_size
    )
    scale_col = 1.0 / math.sqrt(facets * grid_size)
    ramp_cos = (ramp_cos * scale_col)[:, None, :, None, :]
    ramp_sin = (ramp_sin * scale_col)[:, None, :, None, :]
    col_real = jnp.sum(moved[:, :, :, :, 0] * ramp_cos - moved[:, :, :, :, 1] * ramp_sin, 0)
    col_imag = jnp.sum(moved[:, :, :, :, 0] * ramp_sin + moved[:, :, :, :, 1] * ramp_cos, 0)
    image = jnp.stack([col_real, col_imag], 0).astype(jnp.bfloat16)
    image = image.transpose(0, 1, 3, 2, 4).reshape(2 * owners * share, slots * grid_size)
    right = lax.all_gather(image, ("facet", "wa"), axis=0, tiled=True)

    f_ids, t_ids, c_ids, o_ids, r_ids = np.meshgrid(
        np.arange(facets), np.arange(teams), np.arange(2), np.arange(owners), np.arange(share), indexing="ij"
    )
    global_row = ((o_ids * teams + t_ids) * strip_rows + f_ids * share + r_ids).reshape(-1)
    is_imag = c_ids.reshape(-1)
    all_cos, all_sin = table(np.arange(grid_size)[:, None] * global_row[None, :], grid_size, -1.0)
    real_rows = np.where(is_imag == 1, -all_sin, all_cos).reshape(facets, band, -1)
    imag_rows = np.where(is_imag == 1, all_cos, all_sin).reshape(facets, band, -1)
    left_all = np.concatenate([real_rows, imag_rows], 1).astype(jnp.bfloat16)
    left = lax.dynamic_index_in_dim(jnp.asarray(left_all), facet_id, 0, keepdims=False)

    layer_dev = layer_w.shape[0] // teams
    levels = lax.dynamic_slice_in_dim(layer_w, team_id * layer_dev, layer_dev, 0)
    pick = np.zeros((grid_size, grid_size), np.float32)
    pick[v_ids.reshape(-1), np.arange(grid_size)] = 1.0
    ordered = jnp.dot(
        screen_phase,
        jnp.asarray(pick.astype(jnp.bfloat16)).astype(jnp.float32),
        precision=lax.Precision.HIGHEST,
    )
    angles = levels.astype(jnp.float32)[:, None, None] * ordered[None]
    cos = jnp.cos(angles)
    sin = jnp.sin(angles)

    fwd_cos, fwd_sin = table(v_ids[:, :, None] * np.arange(part)[None, None, :], grid_size, -1.0)
    rounded = lambda x: x.astype(jnp.bfloat16).astype(np.float64)
    fwd_cos, fwd_sin = rounded(fwd_cos), rounded(fwd_sin)
    forward = np.concatenate(
        [np.concatenate([fwd_cos, fwd_sin], 2), np.concatenate([-fwd_sin, fwd_cos], 2)], 1
    )
    forward = (forward / math.sqrt(grid_size)).astype(jnp.bfloat16)
    return finish(left, right, cos, sin, jnp.asarray(forward), slots, 1.0 / math.sqrt(strip_total))


def solution(mesh):
    in_specs = (
        P("facet", ("sub", "wa"), None, None),
        P(),
        P("facet", None),
        P(),
        P(),
        P(),
        P(),
        P(),
        P(),
    )
    out_specs = P("sub", "wa", "facet", None, None)
    return jax.shard_map(local, mesh=mesh, in_specs=in_specs, out_specs=out_specs, check_vma=False)
```

```python
import functools
import math

import jax
import jax.numpy as jnp
import numpy as np
from jax import lax
from jax.experimental import pallas as pl
from jax.experimental.pallas import tpu as pltpu
from jax.sharding import PartitionSpec as P

RADIX = 4


def table(products, modulus, sign_value):
    angles = (sign_value * 2.0 * math.pi / modulus) * (products % modulus).astype(np.float64)
    return np.cos(angles), np.sin(angles)


def wave(products, modulus):
    angles = (2.0 * math.pi / modulus) * (products % modulus).astype(jnp.float32)
    return jnp.cos(angles), jnp.sin(angles)


def high(form, left, right):
    return jnp.einsum(form, left, right, precision=lax.Precision.HIGH)


def facet_spectrum(signal):
    strip_rows = signal.shape[0]
    facet_len = signal.shape[2]
    inner_len = 128
    outer_len = facet_len // inner_len
    grid_in = signal.reshape(strip_rows, 2 * outer_len, inner_len)
    outer_ids = np.arange(outer_len)
    inner_ids = np.arange(inner_len)
    c1, s1 = table(outer_ids[:, None] * outer_ids[None, :], outer_len, -1.0)
    first = np.block([[c1, -s1], [s1, c1]]).astype(np.float32)
    mid = high("zy,ryq->rzq", jnp.asarray(first), grid_in)
    mid_real = mid[:, :outer_len]
    mid_imag = mid[:, outer_len:]
    ct, st = table(outer_ids[:, None] * inner_ids[None, :], facet_len, -1.0)
    ct = jnp.asarray(ct.astype(np.float32))
    st = jnp.asarray(st.astype(np.float32))
    turned_real = mid_real * ct - mid_imag * st
    turned_imag = mid_real * st + mid_imag * ct
    turned = jnp.concatenate([turned_real, turned_imag], 2)
    c2, s2 = table(inner_ids[:, None] * inner_ids[None, :], inner_len, -1.0)
    scale = 1.0 / math.sqrt(facet_len)
    second = (np.block([[c2, s2], [-s2, c2]]) * scale).astype(np.float32)
    out = high("rpn,nq->rqp", turned, jnp.asarray(second))
    return out.reshape(strip_rows, 2, facet_len)


def finish_kernel(band, count, scale_rows, left_ref, right_ref, cos_ref, sin_ref, fwd_ref, out_ref, held):
    layer = pl.program_id(1)
    grid_size = cos_ref.shape[2]
    part = grid_size // RADIX

    @pl.when(layer == 0)
    def _():
        rows = jnp.dot(left_ref[...], right_ref[...], preferred_element_type=jnp.float32)
        held[...] = (rows * scale_rows).astype(jnp.bfloat16)

    real = held[:band, :].astype(jnp.float32)
    imag = held[band:, :].astype(jnp.float32)
    cos = cos_ref[0]
    sin = sin_ref[0]
    s_real = (real * cos - imag * sin).astype(jnp.bfloat16)
    s_imag = (real * sin + imag * cos).astype(jnp.bfloat16)
    pieces = []
    for p in range(RADIX):
        lo, hi = p * part, (p + 1) * part
        pair = jnp.concatenate([s_real[:, lo:hi], s_imag[:, lo:hi]], 1)
        got = jnp.dot(pair, fwd_ref[p], preferred_element_type=jnp.float32)
        pieces.append((got[:, :part], got[:, part:]))
    (ar, ai), (br, bi), (cr, ci), (dr, di) = pieces
    er, ei, fr, fi = ar + cr, ai + ci, ar - cr, ai - ci
    gr, gi, hr, hi_ = br + dr, bi + di, br - dr, bi - di
    reals = jnp.concatenate([er + gr, fr + hi_, er - gr, fr - hi_], 1)
    imags = jnp.concatenate([ei + gi, fi - hr, ei - gi, fi + hr], 1)
    out_ref[0, 0, :, 0, :] = reals.astype(jnp.bfloat16)
    out_ref[0, 0, :, 1, :] = imags.astype(jnp.bfloat16)


def finish(left, right, cos, sin, forward, slots, scale_rows):
    layers, band, grid_size = cos.shape
    count = right.shape[0]
    return pl.pallas_call(
        functools.partial(finish_kernel, band, count, scale_rows),
        grid=(slots, layers),
        out_shape=jax.ShapeDtypeStruct((slots, layers, band, 2, grid_size), jnp.bfloat16),
        in_specs=[
            pl.BlockSpec((2 * band, count), lambda s, l: (0, 0)),
            pl.BlockSpec((count, grid_size), lambda s, l: (0, s)),
            pl.BlockSpec((1, band, grid_size), lambda s, l: (l, 0, 0)),
            pl.BlockSpec((1, band, grid_size), lambda s, l: (l, 0, 0)),
            pl.BlockSpec(forward.shape, lambda s, l: (0, 0, 0)),
        ],
        out_specs=pl.BlockSpec((1, 1, band, 2, grid_size), lambda s, l: (s, l, 0, 0, 0)),
        scratch_shapes=[pltpu.VMEM((2 * band, grid_size), jnp.bfloat16)],
        compiler_params=pltpu.CompilerParams(vmem_limit_bytes=48 * 1024 * 1024),
        cost_estimate=pl.CostEstimate(flops=10_000_000_000, bytes_accessed=20_000_000, transcendentals=0),
    )(left, right, cos, sin, forward)


def doubled(block, axis, size, steps):
    order = [0]
    for step in steps:
        other = lax.ppermute(block, axis, [(i, i ^ step) for i in range(size)])
        block = jnp.concatenate([block, other], 0)
        order = order + [o ^ step for o in order]
    return block, order


def local(
    facet_data,
    window,
    screen_phase,
    facet_shift,
    sub_offset,
    win_start,
    win_extent,
    owner_slot,
    layer_w,
):
    facets = lax.axis_size("facet")
    owners = lax.axis_size("sub")
    teams = lax.axis_size("wa")
    facet_id = lax.axis_index("facet")
    team_id = lax.axis_index("wa")
    strip_rows = facet_data.shape[1]
    facet_len = facet_data.shape[3]
    band = screen_phase.shape[0]
    grid_size = screen_phase.shape[1]
    width = grid_size // 2
    part = grid_size // RADIX
    total_subs = owner_slot.shape[0]
    slots = total_subs // owners
    share = strip_rows // facets
    strip_total = strip_rows * owners * teams

    spectrum = facet_spectrum(facet_data[0].astype(jnp.float32) * window)
    slot_ids = jnp.arange(total_subs, dtype=jnp.int32)
    chooser = (owner_slot[None, :] == slot_ids[:, None]).astype(jnp.int32)
    offset_slot = jnp.sum(chooser * sub_offset[None, :], axis=1)
    start_all = jnp.sum(win_start[:, None, :] * chooser[None], axis=2)
    extent_all = jnp.sum(win_extent[:, None, :] * chooser[None], axis=2)
    start_mine = lax.dynamic_index_in_dim(start_all, facet_id, 0, keepdims=False)
    extent_mine = lax.dynamic_index_in_dim(extent_all, facet_id, 0, keepdims=False)
    shift_value = lax.dynamic_index_in_dim(facet_shift, facet_id, 0, keepdims=False)
    begin = (offset_slot + start_mine) % facet_len
    steps = jnp.arange(width, dtype=jnp.int32)
    turn_cos, turn_sin = wave(shift_value * (start_mine[:, None] + steps[None, :]), grid_size)
    inside = steps[None, :] < extent_mine[:, None]
    turn_cos = jnp.where(inside, turn_cos, 0.0)
    turn_sin = jnp.where(inside, turn_sin, 0.0)
    wrapped = jnp.concatenate([spectrum, spectrum[:, :, :width]], 2)
    cuts = []
    for j in range(total_subs):
        picked = lax.dynamic_slice_in_dim(wrapped, begin[j], width, 2)
        cos_j = turn_cos[j][None, :]
        sin_j = turn_sin[j][None, :]
        cuts.append(
            jnp.concatenate(
                [
                    picked[:, 0] * cos_j - picked[:, 1] * sin_j,
                    picked[:, 0] * sin_j + picked[:, 1] * cos_j,
                ],
                1,
            ).astype(jnp.bfloat16)
        )
    sendable = jnp.stack(cuts).reshape(owners, slots, facets, share, 2 * width)
    sendable = sendable.transpose(2, 0, 1, 3, 4).reshape(facets * owners, slots * share, 2 * width)
    received = lax.all_to_all(sendable, ("facet", "sub"), split_axis=0, concat_axis=0, tiled=True)

    v_ids = np.arange(part)[None, :] * RADIX + np.arange(RADIX)[:, None]
    back_cos, back_sin = table(np.arange(width)[:, None] * v_ids.reshape(1, -1), grid_size, 1.0)
    back = np.block([[back_cos, back_sin], [-back_sin, back_cos]])
    moved = jnp.dot(
        received.reshape(facets * owners * slots * share, 2 * width),
        jnp.asarray(back.astype(jnp.bfloat16)),
        preferred_element_type=jnp.float32,
    ).reshape(facets, owners, slots, share, 2, grid_size)
    my_slot = lax.axis_index("sub") * slots
    start_slot = lax.dynamic_slice_in_dim(start_all, my_slot, slots, 1)
    ramp_cos, ramp_sin = wave(
        start_slot[:, :, None] * jnp.asarray(v_ids.reshape(1, 1, -1).astype(np.int32)), grid_size
    )
    scale_col = 1.0 / math.sqrt(facets * grid_size)
    ramp_cos = (ramp_cos * scale_col)[:, None, :, None, :]
    ramp_sin = (ramp_sin * scale_col)[:, None, :, None, :]
    col_real = jnp.sum(moved[:, :, :, :, 0] * ramp_cos - moved[:, :, :, :, 1] * ramp_sin, 0)
    col_imag = jnp.sum(moved[:, :, :, :, 0] * ramp_sin + moved[:, :, :, :, 1] * ramp_cos, 0)
    image = jnp.stack([col_real, col_imag], 0).astype(jnp.bfloat16)
    image = image.transpose(0, 1, 3, 2, 4).reshape(2 * owners * share, slots * grid_size)
    facet_steps = [1 << i for i in range(facets.bit_length() - 1)]
    team_steps = [1 << i for i in range(teams.bit_length() - 1)][::-1]
    right, facet_order = doubled(image, "facet", facets, facet_steps)
    right, team_order = doubled(right, "wa", teams, team_steps)

    me_f, me_t, t_ids, f_ids, c_ids, o_ids, r_ids = np.meshgrid(
        np.arange(facets), np.arange(teams), np.array(team_order), np.array(facet_order),
        np.arange(2), np.arange(owners), np.arange(share), indexing="ij"
    )
    global_row = (o_ids * teams + (t_ids ^ me_t)) * strip_rows + (f_ids ^ me_f) * share + r_ids
    global_row = global_row.reshape(facets, teams, 1, -1)
    is_imag = c_ids.reshape(facets, teams, 1, -1)
    my_rows = np.arange(grid_size).reshape(facets, 1, band, 1)
    all_cos, all_sin = table(my_rows * global_row, grid_size, -1.0)
    real_rows = np.where(is_imag == 1, -all_sin, all_cos)
    imag_rows = np.where(is_imag == 1, all_cos, all_sin)
    left_all = np.concatenate([real_rows, imag_rows], 2).astype(jnp.bfloat16)
    left_all = left_all.reshape(facets * teams, 2 * band, -1)
    left = lax.dynamic_index_in_dim(jnp.asarray(left_all), facet_id * teams + team_id, 0, keepdims=False)

    layer_dev = layer_w.shape[0] // teams
    levels = lax.dynamic_slice_in_dim(layer_w, team_id * layer_dev, layer_dev, 0)
    pick = np.zeros((grid_size, grid_size), np.float32)
    pick[v_ids.reshape(-1), np.arange(grid_size)] = 1.0
    ordered = jnp.dot(
        screen_phase,
        jnp.asarray(pick.astype(jnp.bfloat16)).astype(jnp.float32),
        precision=lax.Precision.HIGHEST,
    )
    angles = levels.astype(jnp.float32)[:, None, None] * ordered[None]
    cos = jnp.cos(angles)
    sin = jnp.sin(angles)

    fwd_cos, fwd_sin = table(v_ids[:, :, None] * np.arange(part)[None, None, :], grid_size, -1.0)
    rounded = lambda x: x.astype(jnp.bfloat16).astype(np.float64)
    fwd_cos, fwd_sin = rounded(fwd_cos), rounded(fwd_sin)
    forward = np.concatenate(
        [np.concatenate([fwd_cos, fwd_sin], 2), np.concatenate([-fwd_sin, fwd_cos], 2)], 1
    )
    forward = (forward / math.sqrt(grid_size)).astype(jnp.bfloat16)
    return finish(left, right, cos, sin, jnp.asarray(forward), slots, 1.0 / math.sqrt(strip_total))


def solution(mesh):
    in_specs = (
        P("facet", ("sub", "wa"), None, None),
        P(),
        P("facet", None),
        P(),
        P(),
        P(),
        P(),
        P(),
        P(),
    )
    out_specs = P("sub", "wa", "facet", None, None)
    return jax.shard_map(local, mesh=mesh, in_specs=in_specs, out_specs=out_specs, check_vma=False)
```
